32 devices in a mesh: section: 4 (over y, x), tensor: 8 (over z, core).
Axes of the slice: x: 2, y: 2, z: 4, core: 2. Of those that a mesh axis runs over, the one named last changes fastest.
Arguments:
- token_ids: int32 [3, 48], replicated, may hold values from 0 to 31999
- emb_table: bfloat16 [32000, 4096], P('section', 'tensor'), may hold values from -6 to 6
- attn_gain: bfloat16 [4, 4096], P('section'), may hold values from 0.25 to 1.75
- query_weight: bfloat16 [4, 4096, 4096], P('section', None, 'tensor'), may hold values from -8 to 8
- key_weight: bfloat16 [4, 4096, 4096], P('section', None, 'tensor'), may hold values from -8 to 8
- value_weight: bfloat16 [4, 4096, 4096], P('section', None, 'tensor'), may hold values from -0.09375 to 0.09375
- mix_weight: float32 [4, 32], P('section', 'tensor'), may hold values from 0.2 to 0.8
- out_weight: bfloat16 [4, 4096, 4096], P('section', 'tensor'), may hold values from -0.125 to 0.125
Outputs:
- layer_outputs: bfloat16 [4, 3, 48, 4096], P('section', None, None, 'tensor')
The draws below stay inside these ranges and needn't reach their ends.
All inputs are finite; a program needn't handle non-finite values.
Results may differ from the reference program's by a relative error of at most 0.033.
Values may be sent and summed in bfloat16 or wider, within the bound.
A program may use at most 64 MiB of HBM per device.

```python
import jax
import jax.numpy as jnp
from jax import lax

D = 4096
HEADS = 32
HEAD_DIM = 128
VOCAB = 32000
MICRO = 3
SEQ = 48
LAYERS = 4
N_TENSOR = 8


def weight_pair(key):
    query_key = jax.random.fold_in(key, 101)
    other_key = jax.random.fold_in(key, 202)
    shape = (LAYERS, D, HEADS * HEAD_DIM)
    base_draw = jax.random.normal(query_key, shape, jnp.float32) * D ** (-0.5)
    other_draw = jax.random.normal(other_key, shape, jnp.float32) * D ** (-0.5)
    return (base_draw, other_draw)


def draw_query_weight(key, part):
    return jnp.clip(weight_pair(key)[0], -8.0, 8.0).astype(jnp.bfloat16)


def draw_key_weight(key, part):
    return jnp.clip(weight_pair(key)[1], -8.0, 8.0).astype(jnp.bfloat16)


def plant(drawn, own_key, low, top_value):
    dims = drawn.shape
    spot = [jax.random.randint(jax.random.fold_in(own_key, axis), (), 0, dims[axis]) for axis in range(len(dims))]
    drawn = drawn.at[tuple(spot)].set(low)
    longest = dims.index(max(dims))
    spot[longest] = (spot[longest] + 1) % dims[longest]
    return drawn.at[tuple(spot)].set(top_value)


def strengthened(result, key, source, target, parts, factor):
    def block_of(axis_at):
        return (jnp.arange(result.shape[axis_at]) // (result.shape[axis_at] // parts)).reshape((-1,) + (1,) * (result.ndim - 1 - axis_at))

    near = jax.random.permutation(key, parts)[block_of(target)]
    other_side = (block_of(target) + parts // 2) % parts
    return jnp.where((block_of(source) == near) | (block_of(source) == other_side), factor * result, result)


def block_levels(key, dims, pieces, least, top_value):
    loudness = 1.0
    for axis_at, parts in pieces:
        heights = jax.random.uniform(jax.random.fold_in(jax.random.fold_in(key, 6), axis_at), (parts,), jnp.float32, least / len(pieces), top_value / len(pieces))
        loudness = loudness * jnp.repeat(jnp.exp(heights), dims[axis_at] // parts).reshape((-1,) + (1,) * (len(dims) - 1 - axis_at))
    return loudness


def normal_values(rng, extent, scale, limit, cuts=(), held_as=jnp.bfloat16):
    drawn = jax.random.normal(rng, extent, jnp.float32) * scale
    if len(cuts) > 0:
        drawn = block_levels(rng, extent, cuts, -0.22, 0.18) * drawn
    return jnp.clip(drawn, min=-limit, max=limit).astype(held_as)


def heavy_noise(key, extent, width, bound, cuts, heavy, kind=jnp.bfloat16):
    array = width * jax.random.normal(key, extent, jnp.float32)
    if cuts:
        array = array * block_levels(key, extent, cuts, -0.22, 0.18)
    return jnp.clip(strengthened(array, jax.random.fold_in(key, 3), *heavy), -bound, bound).astype(kind)


def setup_inputs(seed: int = 0) -> dict:
    streams_of = jax.random.split(jax.random.key(seed), 9)
    token_ids = plant(jax.random.randint(streams_of[0], (MICRO, SEQ), 0, VOCAB), jax.random.fold_in(streams_of[0], 1), 0, VOCAB - 1).astype(jnp.int32)
    emb_table = normal_values(streams_of[1], (VOCAB, D), 1.0, 6.0, ((0, 4), (1, 8)))
    attn_gain = jnp.clip(1.0 + 0.15 * jax.random.normal(streams_of[2], (LAYERS, D), jnp.float32), 0.25, 1.75).astype(jnp.bfloat16)
    query_weight = draw_query_weight(jax.random.fold_in(streams_of[8], 71), 0)
    key_weight = draw_key_weight(jax.random.fold_in(streams_of[8], 71), 0)
    value_weight = normal_values(streams_of[5], (LAYERS, D, HEADS * HEAD_DIM), D ** -0.5, 0.09375, ((0, 4), (2, 8)))
    mix_weight = jnp.clip(0.2 + 0.6 * jax.random.uniform(streams_of[6], (LAYERS, HEADS), jnp.float32) ** block_levels(streams_of[6], (LAYERS, HEADS), ((0, 4), (1, 8)), -0.2, 0.2), 0.2, 0.8)
    out_weight = heavy_noise(streams_of[7], (LAYERS, HEADS * HEAD_DIM, D), (HEADS * HEAD_DIM) ** -0.5, 0.125, ((0, 4), (1, 8)), (1, 2, 8, 2.0))
    return {"token_ids": token_ids, "emb_table": emb_table, "attn_gain": attn_gain, "query_weight": query_weight, "key_weight": key_weight, "value_weight": value_weight, "mix_weight": mix_weight, "out_weight": out_weight}


EPSILON = 1e-05
ROTARY_BASE = 10000.0

def rms_scale(values, norm_gain):
    mean_square = lax.optimization_barrier(jnp.mean(values * values, axis=-1, keepdims=True))
    return values * lax.rsqrt(mean_square + EPSILON) * norm_gain

def rotate(values):
    length = values.shape[-3]
    head_dim = values.shape[-1]
    half_dim = head_dim // 2
    positions = jnp.arange(length, dtype=jnp.float32)
    frequency = ROTARY_BASE ** (-(jnp.arange(half_dim, dtype=jnp.float32) * 2.0) / head_dim)
    angles = positions[:, None] * frequency[None, :]
    cosine = jnp.cos(angles)[:, None, :]
    sine_table = jnp.sin(angles)[:, None, :]
    leading = values[..., :half_dim]
    second = values[..., half_dim:]
    return jnp.concatenate([leading * cosine - second * sine_table, second * cosine + leading * sine_table], axis=-1)

def attend(queries, key_rows, mixed_values):
    length = queries.shape[1]
    scores = jnp.einsum('mqhd,mkhd->mhqk', queries.astype(jnp.float32), key_rows.astype(jnp.float32)) * HEAD_DIM ** (-0.5)
    causal = jnp.arange(length)[:, None] >= jnp.arange(length)[None, :]
    scores = jnp.where(causal, scores, -1e+30)
    row_top = lax.optimization_barrier(jnp.max(scores, axis=-1, keepdims=True))
    expo = jnp.exp(scores - row_top)
    attn_probs = (expo / lax.optimization_barrier(jnp.sum(expo, axis=-1, keepdims=True))).astype(jnp.bfloat16)
    attended = jnp.einsum('mhqk,mkhd->mqhd', attn_probs.astype(jnp.float32), mixed_values.astype(jnp.float32))
    return attended.astype(jnp.bfloat16)

def reference(token_ids, emb_table, attn_gain, query_weight, key_weight, value_weight, mix_weight, out_weight):
    batches, length = token_ids.shape
    first_rows = jnp.take(emb_table, token_ids.reshape(-1).astype(jnp.int32), axis=0)
    first_float = first_rows.astype(jnp.float32)
    first_norm = rms_scale(first_float, attn_gain[0].astype(jnp.float32)).astype(jnp.bfloat16)
    first_values = jnp.dot(first_norm, value_weight[0], preferred_element_type=jnp.float32).astype(jnp.bfloat16)
    source_values = first_values.reshape(batches, length, HEADS, HEAD_DIM).astype(jnp.float32)
    hidden = first_rows.reshape(batches, length, D)
    collected = []
    for layer_index in range(LAYERS):
        norm_gain = attn_gain[layer_index].astype(jnp.float32)
        normed = rms_scale(hidden.astype(jnp.float32), norm_gain).astype(jnp.bfloat16).reshape(-1, D)
        queries = jnp.dot(normed, query_weight[layer_index], preferred_element_type=jnp.float32)
        key_rows = jnp.dot(normed, key_weight[layer_index], preferred_element_type=jnp.float32)
        values = jnp.dot(normed, value_weight[layer_index], preferred_element_type=jnp.float32)
        queries = rotate(queries.reshape(batches, length, HEADS, HEAD_DIM)).astype(jnp.bfloat16)
        key_rows = rotate(key_rows.reshape(batches, length, HEADS, HEAD_DIM)).astype(jnp.bfloat16)
        values = values.reshape(batches, length, HEADS, HEAD_DIM)
        mix_rate = mix_weight[layer_index][:, None]
        mixed_values = (mix_rate * values + (1.0 - mix_rate) * source_values).astype(jnp.bfloat16)
        attended = attend(queries, key_rows, mixed_values).reshape(batches, length, N_TENSOR, -1)
        out_groups = out_weight[layer_index].reshape(N_TENSOR, -1, D)
        partial_value = jnp.einsum('msgc,gcd->gmsd', attended.astype(jnp.float32), out_groups.astype(jnp.float32))
        partial_value = lax.optimization_barrier(partial_value.astype(jnp.bfloat16)).astype(jnp.float32)
        summed = lax.optimization_barrier(jnp.sum(partial_value, axis=0))
        hidden = (hidden.astype(jnp.float32) + summed).astype(jnp.bfloat16)
        collected.append(hidden)
    return jnp.stack(collected)
```

```python
import functools

import jax
import jax.numpy as jnp
from jax import lax
from jax.experimental import pallas as pl
from jax.experimental.pallas import tpu as pltpu
from jax.sharding import PartitionSpec as P

EPSILON = 1e-05
ROTARY_BASE = 10000.0
MESH = pl.DeviceIdType.MESH
F32 = jnp.float32
BF16 = jnp.bfloat16


def relay(
    dims,
    looked, gain, cosine, sine, mix, q_hbm, k_hbm, v_hbm, o_hbm,
    out,
    wq, wk, wv, wo, lk, full, fv, part, sib, pair, zr, hid, acc, att,
    w_sem, lk_s, lk_r, ag_s, ag_r, fw_s, fw_r, fv_s, fv_r, sp_s, sp_r, zs_s, zs_r, hp_s,
):
    S, T, B, L, W, heads, head_dim = dims
    Z = T // 2
    width = heads * head_dim
    sec = lax.axis_index("section")
    ten = lax.axis_index("tensor")
    z = lax.div(ten, 2)
    c = lax.rem(ten, 2)
    other = 1 - c
    mate = 2 * z + other
    root = sec == 0
    has_next = sec < S - 1

    def peer(d):
        return lax.rem(z + d, Z)

    def remote(src, dst, send, recv, to_sec, to_ten):
        return pltpu.make_async_remote_copy(
            src_ref=src, dst_ref=dst, send_sem=send, recv_sem=recv,
            device_id=(to_sec, to_ten), device_id_type=MESH,
        )

    def arrived(ref, send, recv):
        remote(ref, ref, send, recv, sec, mate).wait_recv()

    def sent(ref, send, recv):
        remote(ref, ref, send, recv, sec, mate).wait_send()

    loads = [
        pltpu.make_async_copy(hbm.at[0], vmem, w_sem.at[i])
        for i, (hbm, vmem) in enumerate(((q_hbm, wq), (k_hbm, wk), (v_hbm, wv), (o_hbm, wo)))
    ]
    for load in loads:
        load.start()

    barrier = pltpu.get_barrier_semaphore()

    def greet(to_sec, to_ten):
        pl.semaphore_signal(barrier, inc=1, device_id=(to_sec, to_ten), device_id_type=MESH)

    greet(sec, mate)
    for d in range(1, Z):
        greet(sec, 2 * peer(d) + c)

    @pl.when(has_next)
    def _():
        for d in range(Z):
            greet(sec + 1, 2 * peer(d) + c)

    @pl.when(sec > 0)
    def _():
        for d in range(Z):
            greet(sec - 1, 2 * peer(d) + c)
        greet(0, ten)

    @pl.when(root)
    def _():
        for s in range(1, S):
            greet(s, ten)

    greeted = Z + jnp.where(has_next, Z, 0) + jnp.where(root, S - 1, Z + 1)
    pl.semaphore_wait(barrier, greeted)

    @pl.when(sec > 0)
    def _():
        for m in range(B):
            remote(
                looked.at[m], lk.at[m, sec - 1], lk_s.at[m], lk_r.at[m, sec - 1], 0, ten
            ).start()

    @pl.when(root)
    def _():
        for m in range(B):
            rows = looked[m].astype(F32)
            for s in range(S - 1):
                arrived(lk.at[m, s], lk_s.at[m], lk_r.at[m, s])
                rows = rows + lk[m, s].astype(F32)
            full[m, ten] = rows.astype(BF16)
            for d in range(1, Z):
                remote(
                    full.at[m, ten], full.at[m, ten], ag_s.at[m, d], ag_r.at[m, z],
                    sec, 2 * peer(d) + c,
                ).start()

    for load in loads[:3]:
        load.wait()

    def micro(m, carry):
        def block(t, square, first):
            rows = full[m, t].astype(F32)
            span = pl.ds(pl.multiple_of(t * W, W), W)
            scaled = (rows * gain[:, span]).astype(BF16)
            for i, weight in enumerate((wq, wk, wv)):
                product = jnp.dot(scaled, weight[span, :], preferred_element_type=F32)
                if first:
                    acc[i] = product
                else:
                    acc[i] += product
            return square + jnp.sum(rows * rows, axis=-1, keepdims=True)

        square = jnp.zeros((L, 1), F32)
        for d in range(Z):
            from_z = peer(d)
            t = 2 * from_z + c
            if d == 0:
                @pl.when(sec > 0)
                def _():
                    arrived(full.at[m, t], fw_s.at[m, from_z], ag_r.at[m, from_z])
            else:
                arrived(full.at[m, t], fw_s.at[m, from_z], ag_r.at[m, from_z])
            remote(
                full.at[m, t], full.at[m, t], fw_s.at[m, from_z], fw_r.at[m, from_z], sec, mate
            ).start()
            square = block(t, square, d == 0)
        for d in range(Z):
            from_z = peer(d)
            t = 2 * from_z + other
            arrived(full.at[m, t], fw_s.at[m, from_z], fw_r.at[m, from_z])
            square = block(t, square, False)
        scale = lax.rsqrt(square * (1.0 / (T * W)) + EPSILON)

        @pl.when(root)
        def _():
            fv[m] = (acc[2] * scale).astype(BF16)

        @pl.when(sec > 0)
        def _():
            arrived(fv.at[m], fv_s.at[m], fv_r.at[m])

        @pl.when(has_next)
        def _():
            remote(fv.at[m], fv.at[m], fv_s.at[m], fv_r.at[m], sec + 1, ten).start()

        row_at = lax.broadcasted_iota(jnp.int32, (L, L), 0)
        col_at = lax.broadcasted_iota(jnp.int32, (L, L), 1)
        causal = row_at >= col_at
        cos_t = cosine[...]
        sin_t = sine[...]

        def rotated(values):
            turned = pltpu.roll(values, head_dim // 2, 1)
            return (values * cos_t + turned * sin_t).astype(BF16)

        for h in range(heads):
            span = slice(h * head_dim, (h + 1) * head_dim)
            queries = rotated(acc[0, :, span] * scale)
            key_rows = rotated(acc[1, :, span] * scale)
            rate = mix[:, span]
            mixed = (
                rate * (acc[2, :, span] * scale) + (1.0 - rate) * fv[m, :, span].astype(F32)
            ).astype(BF16)
            scores = lax.dot_general(
                queries, key_rows, (((1,), (1,)), ((), ())), preferred_element_type=F32
            ) * head_dim ** (-0.5)
            scores = jnp.where(causal, scores, -1e30)
            expo = jnp.exp(scores - jnp.max(scores, axis=-1, keepdims=True))
            probs = (expo / jnp.sum(expo, axis=-1, keepdims=True)).astype(BF16)
            att[:, span] = jnp.dot(probs, mixed, preferred_element_type=F32).astype(BF16)

        @pl.when(m == 0)
        def _():
            loads[3].wait()

        attended = att[...]
        order = list(range(1, Z)) + [0]

        def projected(t):
            span = pl.ds(pl.multiple_of(t * W, W), W)
            return jnp.dot(attended, wo[:, span], preferred_element_type=F32).astype(BF16)

        for d in order:
            to_z = peer(d)
            part[m, to_z] = projected(2 * to_z + other)
            remote(
                part.at[m, to_z], sib.at[m, to_z], sp_s.at[m, to_z], sp_r.at[m, to_z], sec, mate
            ).start()
        total = full[m, ten].astype(F32)
        for d in order:
            to_z = peer(d)
            mine = projected(2 * to_z + c).astype(F32)
            arrived(sib.at[m, to_z], sp_s.at[m, to_z], sp_r.at[m, to_z])
            mine = mine + sib[m, to_z].astype(F32)
            if d == 0:
                total = total + mine
            else:
                pair[m, to_z] = mine.astype(BF16)
                remote(
                    pair.at[m, to_z], zr.at[m, z], zs_s.at[m, to_z], zs_r.at[m, z],
                    sec, 2 * to_z + c,
                ).start()
        for d in range(1, Z):
            from_z = peer(d)
            arrived(zr.at[m, from_z], zs_s.at[m, from_z], zs_r.at[m, from_z])
            total = total + zr[m, from_z].astype(F32)
        fresh = total.astype(BF16)
        out[0, m] = fresh
        hid[m] = fresh

        @pl.when(has_next)
        def _():
            for d in range(Z):
                remote(
                    hid.at[m], full.at[m, ten], hp_s.at[m, d], ag_r.at[m, z],
                    sec + 1, 2 * peer(d) + c,
                ).start()

        return carry

    lax.fori_loop(0, B, micro, 0)

    def drain(m, carry):
        for d in range(Z):
            at = peer(d)
            sent(full.at[m, 2 * at + c], fw_s.at[m, at], fw_r.at[m, at])
            sent(part.at[m, at], sp_s.at[m, at], sp_r.at[m, at])
            if d > 0:
                sent(pair.at[m, at], zs_s.at[m, at], zs_r.at[m, at])

        @pl.when(root)
        def _():
            for d in range(1, Z):
                sent(full.at[m, ten], ag_s.at[m, d], ag_r.at[m, z])

        @pl.when(sec > 0)
        def _():
            sent(looked.at[m], lk_s.at[m], lk_r.at[m, 0])

        @pl.when(has_next)
        def _():
            sent(fv.at[m], fv_s.at[m], fv_r.at[m])
            for d in range(Z):
                sent(hid.at[m], hp_s.at[m, d], ag_r.at[m, z])

        return carry

    lax.fori_loop(0, B, drain, 0)


def rotary_tables(length, head_dim):
    half_dim = head_dim // 2
    positions = jnp.arange(length, dtype=F32)
    frequency = ROTARY_BASE ** (-(jnp.arange(half_dim, dtype=F32) * 2.0) / head_dim)
    angles = positions[:, None] * frequency[None, :]
    cosine, sine = jnp.cos(angles), jnp.sin(angles)
    return jnp.concatenate([cosine, cosine], -1), jnp.concatenate([-sine, sine], -1)


def shards(
    sections, tensors,
    token_ids, emb_table, attn_gain, query_weight, key_weight, value_weight, mix_weight, out_weight,
):
    section_rank = lax.axis_index("section")
    batches, length = token_ids.shape
    vocab_local, width_local = emb_table.shape
    heads = mix_weight.shape[1]
    width = query_weight.shape[2]
    head_dim = width // heads
    features = query_weight.shape[1]
    flat_ids = token_ids.reshape(-1) - section_rank * vocab_local
    one_hot = (flat_ids[:, None] == jnp.arange(vocab_local, dtype=jnp.int32)[None, :]).astype(BF16)
    looked = jnp.dot(one_hot, emb_table, preferred_element_type=F32).astype(BF16)
    looked = looked.reshape(batches, length, width_local)
    cosine, sine = rotary_tables(length, head_dim)
    mix = jnp.repeat(mix_weight, head_dim, axis=1)
    S, T, B, L, W = sections, tensors, batches, length, width_local
    Z = T // 2
    vmem = pl.BlockSpec(memory_space=pltpu.VMEM)
    hbm = pl.BlockSpec(memory_space=pl.ANY)
    dma = pltpu.SemaphoreType.DMA
    blocks = pltpu.VMEM((B, Z, L, W), BF16)
    return pl.pallas_call(
        functools.partial(relay, (S, T, B, L, W, heads, head_dim)),
        out_shape=jax.ShapeDtypeStruct((1, B, L, W), BF16),
        in_specs=[vmem] * 5 + [hbm] * 4,
        out_specs=vmem,
        scratch_shapes=[
            pltpu.VMEM((features, width), BF16),
            pltpu.VMEM((features, width), BF16),
            pltpu.VMEM((features, width), BF16),
            pltpu.VMEM((width, features), BF16),
            pltpu.VMEM((B, max(S - 1, 1), L, W), BF16),
            pltpu.VMEM((B, T, L, W), BF16),
            pltpu.VMEM((B, L, width), BF16),
            blocks, blocks, blocks, blocks,
            pltpu.VMEM((B, L, W), BF16),
            pltpu.VMEM((3, L, width), F32),
            pltpu.VMEM((L, width), BF16),
            dma((4,)), dma((B,)), dma((B, S)),
            dma((B, Z)), dma((B, Z)), dma((B, Z)), dma((B, Z)),
            dma((B,)), dma((B,)),
            dma((B, Z)), dma((B, Z)), dma((B, Z)), dma((B, Z)), dma((B, Z)),
        ],
        compiler_params=pltpu.CompilerParams(
            collective_id=0, has_side_effects=True, vmem_limit_bytes=48 * 1024 * 1024
        ),
    )(looked, attn_gain.astype(F32), cosine, sine, mix, query_weight, key_weight, value_weight, out_weight)


def solution(mesh):
    in_specs = (
        P(),
        P("section", "tensor"),
        P("section", None),
        P("section", None, "tensor"),
        P("section", None, "tensor"),
        P("section", None, "tensor"),
        P("section", "tensor"),
        P("section", "tensor", None),
    )
    out_specs = P("section", None, None, "tensor")
    body = functools.partial(shards, mesh.shape["section"], mesh.shape["tensor"])
    return jax.shard_map(body, mesh=mesh, in_specs=in_specs, out_specs=out_specs, check_vma=False)
```

```python
import functools

import jax
import jax.numpy as jnp
import numpy as np
from jax import lax
from jax.experimental import pallas as pl
from jax.experimental.pallas import tpu as pltpu
from jax.sharding import PartitionSpec as P

EPSILON = 1e-05
ROTARY_BASE = 10000.0
MESH = pl.DeviceIdType.MESH
F32 = jnp.float32
BF16 = jnp.bfloat16


def relay(
    dims,
    looked, gain, cosine, sine, mix, q_hbm, k_hbm, v_hbm, o_hbm,
    out,
    wq, wk, wv, wo, lk, full, fv, part, sib, pair, zr, hid, acc, att, own, scales,
    w_sem, lk_s, lk_r, ag_s, ag_r, fw_s, fw_r, fv_s, fv_r, sp_s, sp_r, zs_s, zs_r, hp_s,
):
    S, T, B, C, L, W, heads, head_dim = dims
    Z = T // 2
    Wc = W // C
    sec = lax.axis_index("section")
    ten = lax.axis_index("tensor")
    z = lax.div(ten, 2)
    c = lax.rem(ten, 2)
    other = 1 - c
    mate = 2 * z + other
    root = sec == 0
    has_next = sec < S - 1

    def peer(d):
        return lax.rem(z + d, Z)

    def remote(src, dst, send, recv, to_sec, to_ten):
        return pltpu.make_async_remote_copy(
            src_ref=src, dst_ref=dst, send_sem=send, recv_sem=recv,
            device_id=(to_sec, to_ten), device_id_type=MESH,
        )

    def arrived(ref, send, recv):
        remote(ref, ref, send, recv, sec, mate).wait_recv()

    def sent(ref, send, recv):
        remote(ref, ref, send, recv, sec, mate).wait_send()

    loads = [
        pltpu.make_async_copy(hbm.at[0], vmem, w_sem.at[i])
        for i, (hbm, vmem) in enumerate(((q_hbm, wq), (k_hbm, wk), (v_hbm, wv), (o_hbm, wo)))
    ]
    for load in loads:
        load.start()

    barrier = pltpu.get_barrier_semaphore()

    def greet(to_sec, to_ten):
        pl.semaphore_signal(barrier, inc=1, device_id=(to_sec, to_ten), device_id_type=MESH)

    greet(sec, mate)
    for d in range(1, Z):
        greet(sec, 2 * peer(d) + c)

    @pl.when(has_next)
    def _():
        for d in range(Z):
            greet(sec + 1, 2 * peer(d) + c)

    @pl.when(sec > 0)
    def _():
        for d in range(Z):
            greet(sec - 1, 2 * peer(d) + c)
        greet(0, ten)

    @pl.when(root)
    def _():
        for s in range(1, S):
            greet(s, ten)

    greeted = Z + jnp.where(has_next, Z, 0) + jnp.where(root, S - 1, Z + 1)
    pl.semaphore_wait(barrier, greeted)

    @pl.when(sec > 0)
    def _():
        for m in range(B):
            remote(
                looked.at[m], lk.at[m, sec - 1], lk_s.at[m], lk_r.at[m, sec - 1], 0, ten
            ).start()

    @pl.when(root)
    def _():
        for m in range(B):
            rows = looked[m].astype(F32)
            for s in range(S - 1):
                arrived(lk.at[m, s], lk_s.at[m], lk_r.at[m, s])
                rows = rows + lk[m, s].astype(F32)
            for ch in range(C):
                full[m, ten, ch] = rows[:, ch * Wc:(ch + 1) * Wc].astype(BF16)
            for ch in range(C):
                for d in range(1, Z):
                    remote(
                        full.at[m, ten, ch], full.at[m, ten, ch],
                        ag_s.at[m, d, ch], ag_r.at[m, z, ch], sec, 2 * peer(d) + c,
                    ).start()

    for load in loads[:3]:
        load.wait()

    def project(m):
        def block(t, ch, square, first):
            rows = full[m, t, ch].astype(F32)
            span = pl.ds(pl.multiple_of(t * W + ch * Wc, Wc), Wc)
            scaled = (rows * gain[:, span].astype(F32)).astype(BF16)
            for i, weight in enumerate((wq, wk, wv)):
                product = jnp.dot(scaled, weight[span, :], preferred_element_type=F32)
                if first:
                    acc[i] = product
                else:
                    acc[i] += product
            return square + jnp.sum(rows * rows, axis=-1, keepdims=True)

        square = jnp.zeros((L, 1), F32)
        for ch in range(C):
            for d in range(Z):
                from_z = peer(d)
                t = 2 * from_z + c
                here = full.at[m, t, ch]

                def landed():
                    arrived(here, fw_s.at[m, from_z, ch], ag_r.at[m, from_z, ch])

                if d == 0:
                    pl.when(sec > 0)(landed)
                else:
                    landed()
                remote(
                    here, here, fw_s.at[m, from_z, ch], fw_r.at[m, from_z, ch], sec, mate
                ).start()
                square = block(t, ch, square, d == 0 and ch == 0)
        for ch in range(C):
            for d in range(Z):
                from_z = peer(d)
                t = 2 * from_z + other
                arrived(full.at[m, t, ch], fw_s.at[m, from_z, ch], fw_r.at[m, from_z, ch])
                square = block(t, ch, square, False)
        scale = lax.rsqrt(square * (1.0 / (T * W)) + EPSILON)
        scales[...] = jnp.broadcast_to(scale, scales.shape)

    order = list(range(1, Z)) + [0]

    def attend(m):
        scale = scales[...]

        @pl.when(root)
        def _():
            for h in range(heads):
                span = slice(h * head_dim, (h + 1) * head_dim)
                fv[m, :, span] = (acc[2, :, span] * scale).astype(BF16)

        @pl.when(sec > 0)
        def _():
            arrived(fv.at[m], fv_s.at[m], fv_r.at[m])

        @pl.when(has_next)
        def _():
            remote(fv.at[m], fv.at[m], fv_s.at[m], fv_r.at[m], sec + 1, ten).start()

        row_at = lax.broadcasted_iota(jnp.int32, (L, L), 0)
        col_at = lax.broadcasted_iota(jnp.int32, (L, L), 1)
        causal = row_at >= col_at
        cos_t = cosine[...]
        sin_t = sine[...]

        def rotated(values):
            turned = pltpu.roll(values, head_dim // 2, 1)
            return (values * cos_t + turned * sin_t).astype(BF16)

        for h in range(heads):
            span = slice(h * head_dim, (h + 1) * head_dim)
            queries = rotated(acc[0, :, span] * scale)
            key_rows = rotated(acc[1, :, span] * scale)
            rate = mix[0:1, h:h + 1]
            mixed = (
                rate * (acc[2, :, span] * scale) + (1.0 - rate) * fv[m, :, span].astype(F32)
            ).astype(BF16)
            scores = lax.dot_general(
                queries, key_rows, (((1,), (1,)), ((), ())), preferred_element_type=F32
            ) * head_dim ** (-0.5)
            scores = jnp.where(causal, scores, -1e30)
            expo = jnp.exp(scores - jnp.max(scores, axis=-1, keepdims=True))
            probs = (expo / jnp.sum(expo, axis=-1, keepdims=True)).astype(BF16)
            att[:, span] = jnp.dot(probs, mixed, preferred_element_type=F32).astype(BF16)

        @pl.when(m == 0)
        def _():
            loads[3].wait()

        attended = att[...]

        def projected(t, ch):
            span = pl.ds(pl.multiple_of(t * W + ch * Wc, Wc), Wc)
            return jnp.dot(attended, wo[:, span], preferred_element_type=F32).astype(BF16)

        for ch in range(C):
            for d in order:
                to_z = peer(d)
                part[m, to_z, ch] = projected(2 * to_z + other, ch)
                remote(
                    part.at[m, to_z, ch], sib.at[m, to_z, ch],
                    sp_s.at[m, to_z, ch], sp_r.at[m, to_z, ch], sec, mate,
                ).start()
        for ch in range(C):
            for d in order:
                to_z = peer(d)
                mine = projected(2 * to_z + c, ch).astype(F32)
                arrived(sib.at[m, to_z, ch], sp_s.at[m, to_z, ch], sp_r.at[m, to_z, ch])
                mine = mine + sib[m, to_z, ch].astype(F32)
                if d == 0:
                    own[ch] = full[m, ten, ch].astype(F32) + mine
                else:
                    pair[m, to_z, ch] = mine.astype(BF16)
                    remote(
                        pair.at[m, to_z, ch], zr.at[m, z, ch],
                        zs_s.at[m, to_z, ch], zs_r.at[m, z, ch], sec, 2 * to_z + c,
                    ).start()

    def finish(m):
        for ch in range(C):
            total = own[ch]
            for d in range(1, Z):
                from_z = peer(d)
                arrived(zr.at[m, from_z, ch], zs_s.at[m, from_z, ch], zs_r.at[m, from_z, ch])
                total = total + zr[m, from_z, ch].astype(F32)
            fresh = total.astype(BF16)
            hid[m, ch] = fresh

            @pl.when(has_next)
            def _():
                for d in range(Z):
                    remote(
                        hid.at[m, ch], full.at[m, ten, ch], hp_s.at[m, d, ch], ag_r.at[m, z, ch],
                        sec + 1, 2 * peer(d) + c,
                    ).start()

            out[0, m, :, ch * Wc:(ch + 1) * Wc] = fresh

    def step(m, carry):
        @pl.when(m < B)
        def _():
            project(m)

        @pl.when(m > 0)
        def _():
            finish(m - 1)

        @pl.when(m < B)
        def _():
            attend(m)

        return carry

    lax.fori_loop(0, B + 1, step, 0)

    def drain(m, carry):
        for ch in range(C):
            for d in range(Z):
                at = peer(d)
                sent(full.at[m, 2 * at + c, ch], fw_s.at[m, at, ch], fw_r.at[m, at, ch])
                sent(part.at[m, at, ch], sp_s.at[m, at, ch], sp_r.at[m, at, ch])
                if d > 0:
                    sent(pair.at[m, at, ch], zs_s.at[m, at, ch], zs_r.at[m, at, ch])

        @pl.when(root)
        def _():
            for ch in range(C):
                for d in range(1, Z):
                    sent(full.at[m, ten, ch], ag_s.at[m, d, ch], ag_r.at[m, z, ch])

        @pl.when(sec > 0)
        def _():
            sent(looked.at[m], lk_s.at[m], lk_r.at[m, 0])

        @pl.when(has_next)
        def _():
            sent(fv.at[m], fv_s.at[m], fv_r.at[m])
            for ch in range(C):
                for d in range(Z):
                    sent(hid.at[m, ch], hp_s.at[m, d, ch], ag_r.at[m, z, ch])

        return carry

    lax.fori_loop(0, B, drain, 0)


def rotary_tables(length, head_dim):
    half_dim = head_dim // 2
    positions = np.arange(length, dtype=np.float32)
    frequency = ROTARY_BASE ** (-(np.arange(half_dim, dtype=np.float64) * 2.0) / head_dim)
    angles = positions[:, None] * frequency.astype(np.float32)[None, :]
    cosine, sine = np.cos(angles), np.sin(angles)
    tables = np.concatenate([cosine, cosine], -1), np.concatenate([-sine, sine], -1)
    return tuple(jnp.asarray(table, F32) for table in tables)


def shards(
    sections, tensors,
    token_ids, emb_table, attn_gain, query_weight, key_weight, value_weight, mix_weight, out_weight,
):
    section_rank = lax.axis_index("section")
    batches, length = token_ids.shape
    vocab_local, width_local = emb_table.shape
    heads = mix_weight.shape[1]
    width = query_weight.shape[2]
    head_dim = width // heads
    features = query_weight.shape[1]
    flat_ids = token_ids.reshape(-1) - section_rank * vocab_local
    one_hot = (flat_ids[:, None] == jnp.arange(vocab_local, dtype=jnp.int32)[None, :]).astype(BF16)
    looked = jnp.dot(one_hot, emb_table, preferred_element_type=F32).astype(BF16)
    looked = looked.reshape(batches, length, width_local)
    cosine, sine = rotary_tables(length, head_dim)
    S, T, B, L, W = sections, tensors, batches, length, width_local
    Z = T // 2
    C = 2 if W % 256 == 0 else 1
    vmem = pl.BlockSpec(memory_space=pltpu.VMEM)
    hbm = pl.BlockSpec(memory_space=pl.ANY)
    dma = pltpu.SemaphoreType.DMA
    blocks = pltpu.VMEM((B, Z, C, L, W // C), BF16)
    return pl.pallas_call(
        functools.partial(relay, (S, T, B, C, L, W, heads, head_dim)),
        out_shape=jax.ShapeDtypeStruct((1, B, L, W), BF16),
        in_specs=[vmem] * 5 + [hbm] * 4,
        out_specs=vmem,
        scratch_shapes=[
            pltpu.VMEM((features, width), BF16),
            pltpu.VMEM((features, width), BF16),
            pltpu.VMEM((features, width), BF16),
            pltpu.VMEM((width, features), BF16),
            pltpu.VMEM((B, max(S - 1, 1), L, W), BF16),
            pltpu.VMEM((B, T, C, L, W // C), BF16),
            pltpu.VMEM((B, L, width), BF16),
            blocks, blocks, blocks, blocks,
            pltpu.VMEM((B, C, L, W // C), BF16),
            pltpu.VMEM((3, L, width), F32),
            pltpu.VMEM((L, width), BF16),
            pltpu.VMEM((C, L, W // C), F32),
            pltpu.VMEM((L, head_dim), F32),
            dma((4,)), dma((B,)), dma((B, S)),
            dma((B, Z, C)), dma((B, Z, C)), dma((B, Z, C)), dma((B, Z, C)),
            dma((B,)), dma((B,)),
            dma((B, Z, C)), dma((B, Z, C)), dma((B, Z, C)), dma((B, Z, C)), dma((B, Z, C)),
        ],
        compiler_params=pltpu.CompilerParams(
            collective_id=0, has_side_effects=True, vmem_limit_bytes=48 * 1024 * 1024
        ),
    )(looked, attn_gain, cosine, sine, mix_weight, query_weight, key_weight, value_weight, out_weight)


def solution(mesh):
    in_specs = (
        P(),
        P("section", "tensor"),
        P("section", None),
        P("section", None, "tensor"),
        P("section", None, "tensor"),
        P("section", None, "tensor"),
        P("section", "tensor"),
        P("section", "tensor", None),
    )
    out_specs = P("section", None, None, "tensor")
    body = functools.partial(shards, mesh.shape["section"], mesh.shape["tensor"])
    return jax.shard_map(body, mesh=mesh, in_specs=in_specs, out_specs=out_specs, check_vma=False)
```
